256 devices in a mesh: slab: 32 (over z, y), rays: 8 (over x, core).
Axes of the slice: x: 4, y: 4, z: 8, core: 2. Of those that a mesh axis runs over, the one named last changes fastest.
Arguments:
- geometry: float32 [6, 8, 512], P(None, 'rays'), may hold values from -1 to 1
- entry: int32 [32, 8, 512], P('slab', 'rays'), may hold values from 0 to 255
- counts: int32 [32, 8, 512], P('slab', 'rays'), may hold values from 0 to 8
- targets: float32 [3, 8, 512], P(None, 'rays', 'slab'), may hold values from 0 to 1
- w_in: float32 [32, 256, 256], P('slab'), may hold values from -0.375 to 0.375
- w_mid: float32 [32, 2, 256, 256], P('slab'), may hold values from -0.375 to 0.375
- w_out: float32 [32, 4, 256], P('slab'), may hold values from -0.375 to 0.375
- b_hid: float32 [32, 3, 256], P('slab'), may hold values from -3 to 3
- b_out: float32 [32, 4], P('slab'), may hold values from -3 to 3
- freqs: float32 [32, 3, 128], P('slab'), may hold values from -3 to 3
Outputs:
- pixels: float32 [3, 8, 512], P(None, 'rays', 'slab')
- grad_in: float32 [32, 256, 256], P('slab')
- grad_mid: float32 [32, 2, 256, 256], P('slab')
- grad_out: float32 [32, 4, 256], P('slab')
- grad_hid: float32 [32, 3, 256], P('slab')
- grad_bout: float32 [32, 4], P('slab')
The draws below stay inside these ranges and needn't reach their ends.
Inputs may be any that keep to these rules, and one draw needn't show every extreme that they name: `entry`: the index of a ray's first sample in a slab. `counts`: how many of the 8 slots of a ray lie inside a slab; 0 where the ray misses it.
All inputs are finite; a program needn't handle non-finite values.
Results may differ from the reference program's by a relative error of at most 0.0003.
Values sent between devices are 32-bit elements; how exact they have to be, the bound alone decides.
No kernel may reach another device: no remote copies, remote signals or barrier semaphores. Data moves between devices by JAX's collectives and lax.ppermute only.
A program may use at most 128 MiB of HBM per device.

```python
import math
import jax
import jax.numpy as jnp
from jax import lax

H = 256
FE = 128
MID = 2
SAMP = 8
RAYS_GRP = 512
N_SLAB = 32
N_RAYS = 8


def draw_geometry(key, part):
    key_anchor = jax.random.fold_in(key, 11)
    key_angle = jax.random.fold_in(key, 12)
    key_height = jax.random.fold_in(key, 13)
    shape = (N_RAYS, RAYS_GRP)
    anchor = jax.random.uniform(key_anchor, (3,) + shape, jnp.float32, -1.0, 1.0)
    angle = jax.random.uniform(key_angle, shape, jnp.float32, -math.pi, math.pi)
    upright = jax.random.uniform(key_height, shape, jnp.float32, -1.0, 1.0)
    height = upright
    cycle = jnp.sqrt(jnp.maximum(1.0 - height * height, 0.0))
    direction = jnp.stack([cycle * jnp.cos(angle), cycle * jnp.sin(angle), height], axis=0)
    return jnp.concatenate([anchor, direction], axis=0).astype(jnp.float32)


def draw_freqs(key, part):
    shape = (N_SLAB, 3, FE)
    values = jnp.clip(1.5 * jax.random.normal(jax.random.fold_in(key, 22), shape, jnp.float32), -3.0, 3.0)
    return values.astype(jnp.float32)


def place_ends(entries, key, low, top_value):
    spot = [jax.random.randint(jax.random.fold_in(key, axis), (), 0, length) for axis, length in enumerate(entries.shape)]
    longest = entries.shape.index(max(entries.shape))
    next_to = spot[:longest] + [(spot[longest] + 1) % entries.shape[longest]] + spot[longest + 1:]
    return entries.at[tuple(spot)].set(low).at[tuple(next_to)].set(top_value)


def shard_levels(own_key, dims, split, least, largest):
    def one(position, blocks):
        draws = jax.random.uniform(jax.random.fold_in(jax.random.fold_in(own_key, 6), position), (blocks,), jnp.float32, least / len(split), largest / len(split))
        return jnp.repeat(jnp.exp(draws), dims[position] // blocks).reshape((-1,) + (1,) * (len(dims) - position - 1))

    factor_of = one(*split[0])
    for cut in split[1:]:
        factor_of = factor_of * one(*cut)
    return factor_of


def scatter_about(key, extent, deviation, most, pieces=(), kind=jnp.bfloat16):
    level = shard_levels(key, extent, pieces, -0.22, 0.18) if pieces else 1.0
    values = jax.random.normal(key, extent, jnp.float32) * deviation * level
    return jnp.minimum(jnp.maximum(values, -most), most).astype(kind)


def setup_inputs(seed: int = 0) -> dict:
    keys = jax.random.split(jax.random.key(seed), 11)
    return {
        "geometry": draw_geometry(jax.random.fold_in(keys[10], 71), 0),
        "entry": place_ends(jax.random.randint(keys[1], (N_SLAB, N_RAYS, RAYS_GRP), 0, SAMP * N_SLAB), jax.random.fold_in(keys[1], 1), 0, (SAMP * N_SLAB) - 1).astype(jnp.int32),
        "counts": place_ends(jax.random.randint(keys[2], (N_SLAB, N_RAYS, RAYS_GRP), 0, SAMP + 1), jax.random.fold_in(keys[2], 1), 0, SAMP).astype(jnp.int32),
        "targets": jnp.clip(1.0 * jax.random.uniform(keys[3], (3, N_RAYS, RAYS_GRP), jnp.float32) ** shard_levels(keys[3], (3, N_RAYS, RAYS_GRP), ((1, 8), (2, 32)), -0.2, 0.2), 0.0, 1.0),
        "w_in": scatter_about(keys[4], (N_SLAB, 2 * FE, H), (2 * FE) ** -0.5, 0.375, ((0, 32),), jnp.float32),
        "w_mid": scatter_about(keys[5], (N_SLAB, MID, H, H), H ** -0.5, 0.375, ((0, 32),), jnp.float32),
        "w_out": scatter_about(keys[6], (N_SLAB, 4, H), H ** -0.5, 0.375, ((0, 32),), jnp.float32),
        "b_hid": scatter_about(keys[7], (N_SLAB, MID + 1, H), 0.5, 3.0, ((0, 32),), jnp.float32),
        "b_out": scatter_about(keys[8], (N_SLAB, 4), 0.5, 3.0, ((0, 32),), jnp.float32),
        "freqs": draw_freqs(jax.random.fold_in(keys[10], 71), 0),
    }


HIGH = lax.Precision.HIGHEST

def segment(w_in, w_mid, w_out, b_hid, b_out, freqs, geometry, entry, counts, delta):
    width = geometry.shape[1]
    slots = jnp.arange(SAMP, dtype=jnp.int32)[:, None]
    times = 0.25 * (entry.astype(jnp.float32)[None, :] + slots.astype(jnp.float32) + 0.5)
    places = geometry[0:3, None, :] + times[None] * geometry[3:6, None, :]
    places = places.reshape(3, SAMP * width)
    phase = jnp.einsum('dk,dn->nk', freqs, places, precision=HIGH)
    hidden = jnp.concatenate([jnp.sin(phase), jnp.cos(phase)], axis=1)
    hidden = jax.nn.softplus(jnp.dot(hidden, w_in, precision=HIGH) + b_hid[0])
    for layer in range(MID):
        hidden = jax.nn.softplus(jnp.dot(hidden, w_mid[layer], precision=HIGH) + b_hid[layer + 1])
    result = jnp.einsum('ch,nh->cn', w_out, hidden, precision=HIGH) + b_out[:, None]
    sigma = jax.nn.softplus(result[0]).reshape(SAMP, width)
    colors = jax.nn.sigmoid(result[1:]).reshape(3, SAMP, width)
    alive = slots < counts[None, :]
    depth = jnp.where(alive, sigma * delta, jnp.float32(0.0))
    before = jnp.cumsum(depth, axis=0) - depth
    weights = jnp.exp(-before) * (1.0 - jnp.exp(-depth))
    color = lax.optimization_barrier(jnp.sum(weights[None] * colors, axis=1))
    logtrans = -lax.optimization_barrier(jnp.sum(depth, axis=0))
    return jnp.concatenate([color, logtrans[None]], axis=0)

def composite(segments, targets, factor):
    logtrans = segments[3]
    before = jnp.cumsum(logtrans, axis=0) - logtrans
    shade = jnp.exp(before)
    pixels = lax.optimization_barrier(jnp.sum(shade[None] * segments[:3], axis=1)) + jnp.exp(lax.optimization_barrier(jnp.sum(logtrans, axis=0)))[None]
    loss = factor * jnp.sum((pixels - targets) ** 2)
    return (loss, pixels)

def reference(geometry, entry, counts, targets, w_in, w_mid, w_out, b_hid, b_out, freqs):
    total = N_RAYS * RAYS_GRP
    delta = 3.0 / (SAMP * N_SLAB)
    factor = 1.0 / math.sqrt(3.0 * total)
    flat_geometry = geometry.reshape(6, total)
    flat_targets = targets.reshape(3, total)

    def forward(index):
        return segment(w_in[index], w_mid[index], w_out[index], b_hid[index], b_out[index], freqs[index], flat_geometry, entry[index].reshape(total), counts[index].reshape(total), delta)
    segments = lax.map(forward, jnp.arange(N_SLAB, dtype=jnp.int32))
    segments = jnp.transpose(segments, (1, 0, 2))
    loss, pullback, pixels = jax.vjp(lambda s: composite(s, flat_targets, factor), segments, has_aux=True)
    adjoint = pullback(jnp.ones((), jnp.float32))[0]

    def backward(index):

        def local(params):
            return segment(params[0], params[1], params[2], params[3], params[4], freqs[index], flat_geometry, entry[index].reshape(total), counts[index].reshape(total), delta)
        params = (w_in[index], w_mid[index], w_out[index], b_hid[index], b_out[index])
        unused, pull = jax.vjp(local, params)
        return pull(adjoint[:, index, :])[0]
    grads = lax.map(backward, jnp.arange(N_SLAB, dtype=jnp.int32))
    return (pixels.reshape(3, N_RAYS, RAYS_GRP), grads[0], grads[1], grads[2], grads[3], grads[4])
```

```python
import math

import jax
import jax.numpy as jnp
from jax import lax
from jax.experimental import pallas as pl
from jax.experimental.pallas import tpu as pltpu
from jax.sharding import PartitionSpec as P

H = 256
FE = 128
SAMP = 8
RAYS = 512
OWN = 16
ROWS = 17
SPB = 2
STEPS = SAMP // SPB
F32 = jnp.float32
BF16 = jnp.bfloat16
NT = (((1,), (1,)), ((), ()))


def mm(a, b):
    return jnp.dot(a, b, preferred_element_type=F32)


def mm_nt(a, b):
    return lax.dot_general(a, b, NT, preferred_element_type=F32)


def split(x):
    hi = x.astype(BF16)
    return hi, (x - hi.astype(F32)).astype(BF16)


def sincos(phase):
    turns = jnp.floor(phase * F32(2.0 / math.pi) + F32(0.5))
    r = phase - turns * F32(1.5703125)
    r = r - turns * F32(4.837512969970703125e-4)
    r = r - turns * F32(7.54978995489188216e-8)
    z = r * r
    s = r + r * z * (F32(-1.6666654611e-1) + z * (F32(8.3321608736e-3) + z * F32(-1.9515295891e-4)))
    c = F32(1.0) - F32(0.5) * z + z * z * (
        F32(4.166664568298827e-2) + z * (F32(-1.388731625493765e-3) + z * F32(2.443315711809948e-5))
    )
    k = turns.astype(jnp.int32)
    odd = (k & 1) == 1
    sine = jnp.where(odd, c, s)
    cosine = jnp.where(odd, s, c)
    sine = jnp.where((k & 2) == 2, -sine, sine)
    cosine = jnp.where(((k + 1) & 2) == 2, -cosine, cosine)
    return sine, cosine


def softplus(x):
    u = jnp.exp(-jnp.abs(x))
    w = F32(1.0) + u
    return jnp.maximum(x, F32(0.0)) + (jnp.log(w) + (u - (w - F32(1.0))))


def sigmoid(x):
    u = jnp.exp(-jnp.abs(x))
    return jnp.where(x >= 0, F32(1.0), u) / (F32(1.0) + u)


def column(row):
    return jnp.broadcast_to(row, (8, row.shape[1])).T[:, 0:1]


def forward_kernel(
    me_ref, geo_ref, entry_ref, counts_ref, tgt_ref, win_ref, wmid_ref, wout_ref, bhid_ref, bout_ref, freqs_ref,
    send_ref, out_ref, fh_ref, fl_ref, h1h_ref, h1l_ref, h2h_ref, h2l_ref, h3h_ref, h3l_ref, s1_ref, s2_ref, s3_ref,
    wh, wl, wo, bias, rot, feat, before, color,
    *, delta,
):
    step = pl.program_id(0)

    @pl.when(step == 0)
    def _():
        for i in range(3):
            w = win_ref[0] if i == 0 else wmid_ref[0, i - 1]
            hi, lo = split(w.T)
            wh[i] = hi
            wl[i] = lo
            bias[i] = jnp.broadcast_to(column(bhid_ref[0, i : i + 1, :]), (H, 128))
        w8 = jnp.concatenate([wout_ref[0], jnp.zeros((4, H), F32)], axis=0)
        hi, lo = split(w8)
        wo[...] = jnp.concatenate([hi.astype(F32), lo.astype(F32)], axis=0).astype(BF16)
        ft = jnp.concatenate([freqs_ref[0], jnp.zeros((5, FE), F32)], axis=0).T
        geo = geo_ref[:, 0, :]
        a = ft[:, 0:1] * geo[0:1] + ft[:, 1:2] * geo[1:2] + ft[:, 2:3] * geo[2:3]
        d = ft[:, 0:1] * geo[3:4] + ft[:, 1:2] * geo[4:5] + ft[:, 2:3] * geo[5:6]
        t0 = F32(0.25) * (entry_ref[0].astype(F32) + F32(0.5))
        s, c = sincos(a + t0 * d)
        feat[0:FE] = s
        feat[FE:] = c
        s, c = sincos(F32(0.25) * d)
        rot[0:FE] = s
        rot[FE:] = c
        before[...] = jnp.zeros_like(before)
        color[...] = jnp.zeros_like(color)

    def slot_input(j):
        s, c = feat[0:FE], feat[FE:]
        fh_ref[j, 0:FE], fl_ref[j, 0:FE] = split(s)
        fh_ref[j, FE:], fl_ref[j, FE:] = split(c)
        rs, rc = rot[0:FE], rot[FE:]
        feat[0:FE] = s * rc + c * rs
        feat[FE:] = c * rc - s * rs

    for j in range(SPB):
        slot_input(j)
    srcs = [(fh_ref, fl_ref), (h1h_ref, h1l_ref), (h2h_ref, h2l_ref), (h3h_ref, h3l_ref)]
    sigs = [s1_ref, s2_ref, s3_ref]
    parts = [(j, k) for j in range(SPB) for k in range(2)]
    for i in range(3):
        b = bias[i, :, 0:1]
        for j, k in parts:
            lanes = slice(256 * k, 256 * k + 256)
            hi = srcs[i][0][j, :, lanes]
            lo = srcs[i][1][j, :, lanes]
            x = mm(wh[i], hi) + mm(wh[i], lo) + mm(wl[i], hi) + b
            h = softplus(x)
            sigs[i][j, :, lanes] = jnp.exp(x - h)
            srcs[i + 1][0][j, :, lanes], srcs[i + 1][1][j, :, lanes] = split(h)
    bo = jnp.concatenate([bout_ref[0:1, :], jnp.zeros((1, 124), F32)], axis=1)
    bo = jnp.broadcast_to(bo, (128, 128)).T[0:8, 0:1]
    for j in range(SPB):
        d1 = mm(wo[...], h3h_ref[j])
        d2 = mm(wo[...], h3l_ref[j])
        o = d1[0:8] + d1[8:16] + d2[0:8] + d2[8:16] + bo
        out_ref[j] = o
        alive = step * SPB + j < counts_ref[0]
        depth = jnp.where(alive, softplus(o[0:1]) * F32(delta), F32(0.0))
        bef = before[...]
        w = jnp.exp(-bef) * (F32(1.0) - jnp.exp(-depth))
        color[...] += w * sigmoid(o)
        before[...] = bef + depth

    @pl.when(step == STEPS - 1)
    def _():
        t = tgt_ref[:, 0, :]
        t = jnp.concatenate([t[0:1], t[1:2], t[2:3], jnp.zeros((1, 80), F32)], axis=1)
        t = pltpu.roll(jnp.broadcast_to(t, (8, 128)), lax.rem(me_ref[0], 8) * OWN, 1)[0:1]
        rows = []
        for c in range(4):
            v = color[c + 1 : c + 2] if c < 3 else -before[...]
            rows += [v[:, 128 * q : 128 * q + 128] for q in range(4)]
        rows.append(t)
        value = jnp.concatenate(rows, axis=0)
        for s in range(32):
            send_ref[s * ROWS : (s + 1) * ROWS] = value


def full(shape):
    return pl.BlockSpec(shape, lambda i, n=len(shape): (0,) * n)


def smem():
    return pl.BlockSpec(memory_space=pltpu.SMEM)


def slots(rows):
    return pl.BlockSpec((SPB, rows, RAYS), lambda i: (i, 0, 0))


def forward(me, geo, entry, counts, tgt, w_in, w_mid, w_out, b_hid, b_out, freqs, delta):
    res = [jax.ShapeDtypeStruct((32 * ROWS, 128), F32), jax.ShapeDtypeStruct((SAMP, 8, RAYS), F32)]
    res += [jax.ShapeDtypeStruct((SAMP, H, RAYS), BF16)] * 8 + [jax.ShapeDtypeStruct((SAMP, H, RAYS), F32)] * 3
    return pl.pallas_call(
        lambda *refs: forward_kernel(*refs, delta=delta),
        grid=(STEPS,),
        in_specs=[smem()] + [full(x.shape) for x in (geo, entry, counts, tgt, w_in, w_mid, w_out, b_hid, b_out, freqs)],
        out_specs=[full((32 * ROWS, 128)), slots(8)] + [slots(H)] * 11,
        out_shape=res,
        scratch_shapes=[
            pltpu.VMEM((3, H, H), BF16), pltpu.VMEM((3, H, H), BF16), pltpu.VMEM((16, H), BF16),
            pltpu.VMEM((3, H, 128), F32), pltpu.VMEM((H, RAYS), F32), pltpu.VMEM((H, RAYS), F32),
            pltpu.VMEM((1, RAYS), F32), pltpu.VMEM((8, RAYS), F32),
        ],
        compiler_params=pltpu.CompilerParams(vmem_limit_bytes=60 * 1024 * 1024),
        name="fwd",
    )(me, geo, entry, counts, tgt, w_in, w_mid, w_out, b_hid, b_out, freqs)


def backward_kernel(
    me_ref, recv_ref, counts_ref, win_ref, wmid_ref, wout_ref, out_ref,
    fh_ref, fl_ref, h1h_ref, h1l_ref, h2h_ref, h2l_ref, h3h_ref, h3l_ref, s1_ref, s2_ref, s3_ref,
    pix_ref, mine_ref, other_ref,
    wh, wl, woT, g_all, adj, pixs, acc, bacc, gacc, goacc,
    *, delta, factor,
):
    step = pl.program_id(0)

    @pl.when(step == 0)
    def _():
        me = me_ref[0]
        for i in range(2):
            wh[i], wl[i] = split(wmid_ref[0, i])
        w8 = jnp.concatenate([wout_ref[0], jnp.zeros((4, H), F32)], axis=0)
        hi, lo = split(w8)
        hi, lo = hi.astype(F32), lo.astype(F32)
        woT[...] = jnp.concatenate([hi, hi, lo, jnp.zeros((104, H), F32)], axis=0).T.astype(BF16)
        acc[...] = jnp.zeros_like(acc)
        bacc[...] = jnp.zeros_like(bacc)
        gacc[...] = jnp.zeros_like(gacc)
        goacc[...] = jnp.zeros_like(goacc)
        zero = jnp.zeros((4, 128), F32)
        depth, own, pix, after = zero, zero, [zero] * 3, [zero] * 3
        for s in range(32):
            shade = jnp.exp(depth)
            own = jnp.where(me == s, shade, own)
            late = jnp.where(s > me, F32(1.0), F32(0.0))
            for c in range(3):
                part = shade * recv_ref[s * ROWS + 4 * c : s * ROWS + 4 * c + 4]
                pix[c] = pix[c] + part
                after[c] = after[c] + late * part
            depth = depth + recv_ref[s * ROWS + 12 : s * ROWS + 16]
        through = jnp.exp(depth)
        lane = lax.broadcasted_iota(jnp.int32, (8, 128), 1)
        sub = lax.broadcasted_iota(jnp.int32, (8, 128), 0)
        adj[...] = jnp.zeros_like(adj)
        log_adj = zero
        for c in range(3):
            rows = []
            for q in range(4):
                t = jnp.concatenate(
                    [recv_ref[(8 * q + s) * ROWS + 16 : (8 * q + s) * ROWS + 17] for s in range(8)], axis=0
                )
                if c:
                    t = pltpu.roll(t, 128 - OWN * c, 1)
                t = jnp.where(lax.div(lane, OWN) == sub, t, F32(0.0))
                rows.append(jnp.sum(t, axis=0, keepdims=True))
            target = jnp.concatenate(rows, axis=0)
            pixel = pix[c] + through
            pixs[4 * c : 4 * c + 4] = pixel
            dpix = F32(2.0 * factor) * (pixel - target)
            log_adj = log_adj + dpix * (after[c] + through)
            a = own * dpix
            for q in range(4):
                adj[c + 1 : c + 2, 128 * q : 128 * q + 128] = a[q : q + 1]
        for c in range(3):
            row = pixs[pl.ds(4 * c + lax.div(me, 8), 1), :]
            row = pltpu.roll(jnp.broadcast_to(row, (8, 128)), lax.rem(128 - lax.rem(me, 8) * OWN, 128), 1)
            pix_ref[c] = row[0:1, 0:OWN]
        log_adj = jnp.concatenate([log_adj[q : q + 1] for q in range(4)], axis=1)
        a8 = adj[...]
        counts = counts_ref[0]
        bef = jnp.zeros((1, RAYS), F32)
        ends, weights = [], []
        for j in range(SAMP):
            dep = jnp.where(j < counts, softplus(out_ref[j, 0:1]) * F32(delta), F32(0.0))
            weights.append(jnp.exp(-bef) * (F32(1.0) - jnp.exp(-dep)))
            bef = bef + dep
            ends.append(jnp.exp(-bef))
        later = jnp.zeros((8, RAYS), F32)
        first = lax.broadcasted_iota(jnp.int32, (8, RAYS), 0) == 0
        for j in reversed(range(SAMP)):
            sg = sigmoid(out_ref[j])
            ddep = jnp.sum(a8 * (ends[j] * sg - later), axis=0, keepdims=True) - log_adj
            ddep = jnp.where(j < counts, F32(delta) * ddep, F32(0.0))
            g = jnp.where(first, ddep * sg, a8 * weights[j] * (sg * (F32(1.0) - sg)))
            later = later + weights[j] * sg
            g_all[j] = g

    for j in range(SPB):
        g = g_all[step * SPB + j]
        gacc[...] += g[:, 0:128] + g[:, 128:256] + g[:, 256:384] + g[:, 384:512]
        gh, gl = split(g)
        ghf, glf = gh.astype(F32), gl.astype(F32)
        g16 = jnp.concatenate([ghf, glf], axis=0).astype(BF16)
        d1 = mm_nt(g16, h3h_ref[j])
        d2 = mm_nt(g16, h3l_ref[j])
        goacc[...] += d1[0:8] + d1[8:16] + d2[0:8] + d2[8:16]
        gk = jnp.concatenate([ghf, glf, ghf, jnp.zeros((104, RAYS), F32)], axis=0).astype(BF16)
        dh = mm(woT[...], gk)
        for i, (sg, hh, hl) in enumerate(((s3_ref, h2h_ref, h2l_ref), (s2_ref, h1h_ref, h1l_ref), (s1_ref, fh_ref, fl_ref))):
            dx = dh * sg[j]
            bacc[2 - i] += dx[:, 0:128] + dx[:, 128:256] + dx[:, 256:384] + dx[:, 384:512]
            xh, xl = split(dx)
            acc[2 - i] += mm_nt(hh[j], xh) + mm_nt(hh[j], xl) + mm_nt(hl[j], xh)
            if i < 2:
                dh = mm(wh[1 - i], xh) + mm(wh[1 - i], xl) + mm(wl[1 - i], xh)

    @pl.when(step == STEPS - 1)
    def _():
        core, chip = me_ref[1], me_ref[2]
        for k in range(4):
            q = lax.rem(chip + k, 4)
            for i in range(3):
                rows = pl.ds(96 * k + 32 * i, 32)
                mine_ref[rows] = acc[i, pl.ds((core * 4 + q) * 32, 32), :]
                other_ref[rows] = acc[i, pl.ds(((1 - core) * 4 + q) * 32, 32), :]
        lane = lax.broadcasted_iota(jnp.int32, (8, 128), 1)
        sub = lax.broadcasted_iota(jnp.int32, (8, 128), 0)
        hid = [jnp.sum(bacc[i].T, axis=0, keepdims=True) for i in range(3)]
        gb = jnp.broadcast_to(jnp.sum(gacc[...], axis=1, keepdims=True), (8, 128))
        gb = jnp.sum(jnp.where(lane == sub, gb, F32(0.0)), axis=0, keepdims=True)
        gb = jnp.concatenate([gb, jnp.zeros((1, 128), F32)], axis=1)
        small = jnp.concatenate([goacc[0:4]] + hid + [gb], axis=0)
        mine_ref[384:392] = small
        other_ref[384:392] = small


def backward(ids, recv, counts, w_in, w_mid, w_out, out, residuals, delta, factor):
    half = jax.ShapeDtypeStruct((392, H), F32)
    return pl.pallas_call(
        lambda *refs: backward_kernel(*refs, delta=delta, factor=factor),
        grid=(STEPS,),
        in_specs=[smem()] + [full(x.shape) for x in (recv, counts, w_in, w_mid, w_out, out)] + [slots(H)] * 11,
        out_specs=[full((3, 1, OWN)), full((392, H)), full((392, H))],
        out_shape=[jax.ShapeDtypeStruct((3, 1, OWN), F32), half, half],
        scratch_shapes=[
            pltpu.VMEM((2, H, H), BF16), pltpu.VMEM((2, H, H), BF16), pltpu.VMEM((H, 128), BF16),
            pltpu.VMEM((SAMP, 8, RAYS), F32), pltpu.VMEM((8, RAYS), F32), pltpu.VMEM((16, 128), F32),
            pltpu.VMEM((3, H, H), F32), pltpu.VMEM((3, H, 128), F32), pltpu.VMEM((8, 128), F32), pltpu.VMEM((8, H), F32),
        ],
        compiler_params=pltpu.CompilerParams(vmem_limit_bytes=60 * 1024 * 1024),
        name="bwd",
    )(ids, recv, counts, w_in, w_mid, w_out, out, *residuals)


def place_kernel(ids_ref, *refs):
    own, sib, (gin, gmid) = refs[0:4], refs[4], refs[5:]
    core, chip = ids_ref[1], ids_ref[2]
    for k in range(4):
        q = lax.rem(chip + 4 - k, 4)
        for side in range(2):
            src, base = (own[k], 0) if side == 0 else (sib, 96 * k)
            rows = pl.ds(((core if side == 0 else 1 - core) * 4 + q) * 32, 32)
            gin[0, rows] = src[base : base + 32]
            gmid[0, 0, rows] = src[base + 32 : base + 64]
            gmid[0, 1, rows] = src[base + 64 : base + 96]


def place(ids, own, sib):
    vm = pl.BlockSpec(memory_space=pltpu.VMEM)
    return pl.pallas_call(
        place_kernel,
        in_specs=[smem()] + [vm] * 5,
        out_specs=[vm, vm],
        out_shape=[jax.ShapeDtypeStruct((1, H, H), F32), jax.ShapeDtypeStruct((1, 2, H, H), F32)],
        name="place",
    )(ids, *own, sib)


def shards(geometry, entry, counts, targets, w_in, w_mid, w_out, b_hid, b_out, freqs):
    slabs = lax.axis_size("slab")
    delta = 3.0 / (SAMP * slabs)
    factor = 1.0 / math.sqrt(3.0 * lax.axis_size("rays") * slabs * OWN)
    me = lax.axis_index("slab")
    ray = lax.axis_index("rays")
    ids = jnp.stack([me, lax.rem(ray, 2), lax.div(ray, 2)]).astype(jnp.int32)
    send, out, *residuals = forward(
        ids, geometry, entry, counts, targets, w_in, w_mid, w_out, b_hid, b_out, freqs, delta
    )
    recv = lax.all_to_all(send.reshape(32, 1, ROWS * 128), "slab", 0, 0, tiled=True).reshape(32 * ROWS, 128)
    pixels, mine, other = backward(ids, recv, counts, w_in, w_mid, w_out, out, residuals, delta, factor)
    swap = [(i, i ^ 1) for i in range(8)]
    along = [[(i, (i + 2 * k) % 8) for i in range(8)] for k in range(4)]
    total = mine + lax.ppermute(other, "rays", swap)
    small = total[384:392]
    parts = [jnp.concatenate([total[96 * k : 96 * k + 96], small], axis=0) for k in range(4)]
    got = [lax.ppermute(parts[k], "rays", along[k]) for k in range(1, 4)]
    done = parts[0] + got[0] + got[1] + got[2]
    chunk = done[0:96]
    own = [chunk] + [lax.ppermute(chunk, "rays", along[k]) for k in range(1, 4)]
    sib = lax.ppermute(jnp.concatenate(own, axis=0), "rays", swap)
    grad_in, grad_mid = place(ids, own, sib)
    small = done[96:104]
    return pixels, grad_in, grad_mid, small[None, 0:4], small[None, 4:7], small[7:8, 0:4]


def solution(mesh):
    in_specs = (
        P(None, "rays", None),
        P("slab", "rays", None),
        P("slab", "rays", None),
        P(None, "rays", "slab"),
        P("slab", None, None),
        P("slab", None, None, None),
        P("slab", None, None),
        P("slab", None, None),
        P("slab", None),
        P("slab", None, None),
    )
    out_specs = (
        P(None, "rays", "slab"),
        P("slab", None, None),
        P("slab", None, None, None),
        P("slab", None, None),
        P("slab", None, None),
        P("slab", None),
    )
    return jax.shard_map(shards, mesh=mesh, in_specs=in_specs, out_specs=out_specs, check_vma=False)
```

```python
import math

import jax
import jax.numpy as jnp
from jax import lax
from jax.experimental import pallas as pl
from jax.experimental.pallas import tpu as pltpu
from jax.sharding import PartitionSpec as P

H = 256
FE = 128
SAMP = 8
RAYS = 512
OWN = 16
ROWS = 17
SPB = 2
STEPS = SAMP // SPB
F32 = jnp.float32
LOG2E = 1.4426950408889634
LN2 = 0.6931471805599453
BF16 = jnp.bfloat16
NT = (((1,), (1,)), ((), ()))


def mm(a, b):
    return jnp.dot(a, b, preferred_element_type=F32)


def mm_nt(a, b):
    return lax.dot_general(a, b, NT, preferred_element_type=F32)


def split(x):
    hi = x.astype(BF16)
    return hi, (x - hi.astype(F32)).astype(BF16)


def sincos(phase):
    turns = jnp.floor(phase * F32(2.0 / math.pi) + F32(0.5))
    r = phase - turns * F32(1.5703125)
    r = r - turns * F32(4.837512969970703125e-4)
    r = r - turns * F32(7.54978995489188216e-8)
    z = r * r
    s = r + r * z * (F32(-1.6666654611e-1) + z * (F32(8.3321608736e-3) + z * F32(-1.9515295891e-4)))
    c = F32(1.0) - F32(0.5) * z + z * z * (
        F32(4.166664568298827e-2) + z * (F32(-1.388731625493765e-3) + z * F32(2.443315711809948e-5))
    )
    k = turns.astype(jnp.int32)
    odd = (k & 1) == 1
    sine = jnp.where(odd, c, s)
    cosine = jnp.where(odd, s, c)
    sine = jnp.where((k & 2) == 2, -sine, sine)
    cosine = jnp.where(((k + 1) & 2) == 2, -cosine, cosine)
    return sine, cosine


def softplus(x):
    u = jnp.exp(-jnp.abs(x))
    w = F32(1.0) + u
    return jnp.maximum(x, F32(0.0)) + (jnp.log(w) + (u - (w - F32(1.0))))


def softplus2(x):
    v = jnp.exp2(jnp.minimum(x, F32(100.0)))
    log = lax.log2(F32(1.0 - 2.0**-23) + v)
    return jnp.maximum(jnp.maximum(log, v * (F32(LOG2E) - F32(0.5 * LOG2E) * v)), x)


def sigmoid(x):
    u = jnp.exp(-jnp.abs(x))
    return jnp.where(x >= 0, F32(1.0), u) / (F32(1.0) + u)


def forward_kernel(
    me_ref, geo_ref, entry_ref, counts_ref, tgt_ref, win_ref, wmid_ref, wout_ref, bhid_ref, bout_ref, freqs_ref,
    send_ref, out_ref, fh_ref, fl_ref, h1h_ref, h1l_ref, h2h_ref, h2l_ref, h3h_ref, h3l_ref, s1_ref, s2_ref, s3_ref,
    wcat, wo, bias, rot, feat, before, color,
    *, delta,
):
    step = pl.program_id(0)

    @pl.when(step == 0)
    def _():
        for i in range(3):
            w = win_ref[0] * F32(LOG2E) if i == 0 else wmid_ref[0, i - 1]
            hi, lo = split(w.T)
            wcat[i, :, 0:256] = hi
            wcat[i, :, 256:512] = hi
            wcat[i, :, 512:768] = lo
            bias[i] = jnp.broadcast_to(bhid_ref[i] * F32(LOG2E), (128, H)).T
        w8 = jnp.concatenate([wout_ref[0] * F32(LN2), jnp.zeros((4, H), F32)], axis=0)
        hi, lo = split(w8)
        wo[...] = jnp.concatenate([hi.astype(F32), lo.astype(F32)], axis=0).astype(BF16)
        ft = jnp.concatenate([freqs_ref[0], freqs_ref[1], freqs_ref[2], jnp.zeros((5, FE), F32)], axis=0).T
        geo = geo_ref[:, 0, :]
        a = ft[:, 0:1] * geo[0:1] + ft[:, 1:2] * geo[1:2] + ft[:, 2:3] * geo[2:3]
        d = ft[:, 0:1] * geo[3:4] + ft[:, 1:2] * geo[4:5] + ft[:, 2:3] * geo[5:6]
        t0 = F32(0.25) * (entry_ref[0].astype(F32) + F32(0.5))
        s, c = sincos(a + t0 * d)
        feat[0:FE] = s
        feat[FE:] = c
        s, c = sincos(F32(0.25) * d)
        rot[0:FE] = s
        rot[FE:] = c
        before[...] = jnp.zeros_like(before)
        color[...] = jnp.zeros_like(color)

    n = step * SPB

    def slot_input(j):
        s, c = feat[0:FE], feat[FE:]
        fh_ref[n + j, 0:FE], fl_ref[n + j, 0:FE] = split(s)
        fh_ref[n + j, FE:], fl_ref[n + j, FE:] = split(c)
        rs, rc = rot[0:FE], rot[FE:]
        feat[0:FE] = s * rc + c * rs
        feat[FE:] = c * rc - s * rs

    for j in range(SPB):
        slot_input(j)
    srcs = [(fh_ref, fl_ref), (h1h_ref, h1l_ref), (h2h_ref, h2l_ref), (h3h_ref, h3l_ref)]
    sigs = [s1_ref, s2_ref, s3_ref]
    parts = [(j, k) for j in range(SPB) for k in range(2)]
    for i in range(3):
        b = jnp.concatenate([bias[i], bias[i]], axis=1)
        for j, k in parts:
            lanes = slice(256 * k, 256 * k + 256)
            hi = srcs[i][0][n + j, :, lanes]
            lo = srcs[i][1][n + j, :, lanes]
            x = mm(wcat[i], jnp.concatenate([hi, lo, hi], axis=0)) + b
            h = softplus2(x)
            sigs[i][n + j, :, lanes] = jnp.exp2(x - h)
            srcs[i + 1][0][n + j, :, lanes], srcs[i + 1][1][n + j, :, lanes] = split(h)
    bo = jnp.concatenate([bout_ref[0:1, :], jnp.zeros((1, 124), F32)], axis=1)
    bo = jnp.broadcast_to(bo, (128, 128)).T[0:8, 0:1]
    for j in range(SPB):
        d1 = mm(wo[...], h3h_ref[n + j])
        d2 = mm(wo[...], h3l_ref[n + j])
        o = d1[0:8] + d1[8:16] + d2[0:8] + d2[8:16] + bo
        out_ref[step * SPB + j] = o
        alive = step * SPB + j < counts_ref[0]
        depth = jnp.where(alive, softplus(o[0:1]) * F32(delta), F32(0.0))
        bef = before[...]
        w = jnp.exp(-bef) * (F32(1.0) - jnp.exp(-depth))
        color[...] += w * sigmoid(o)
        before[...] = bef + depth

    @pl.when(step == STEPS - 1)
    def _():
        t = tgt_ref[:, 0, :]
        t = jnp.concatenate([t[0:1], t[1:2], t[2:3], jnp.zeros((1, 80), F32)], axis=1)
        t = pltpu.roll(jnp.broadcast_to(t, (8, 128)), lax.rem(me_ref[0], 8) * OWN, 1)[0:1]
        rows = []
        for c in range(4):
            v = color[c + 1 : c + 2] if c < 3 else -before[...]
            rows += [v[:, 128 * q : 128 * q + 128] for q in range(4)]
        rows.append(t)
        value = jnp.concatenate(rows, axis=0)
        for s in range(32):
            send_ref[s * ROWS : (s + 1) * ROWS] = value


def keep(x):
    return pltpu.with_memory_space_constraint(x, pltpu.VMEM)


def vmem():
    return pl.BlockSpec(memory_space=pltpu.VMEM)


def full(shape):
    return pl.BlockSpec(shape, lambda i, n=len(shape): (0,) * n)


def smem():
    return pl.BlockSpec(memory_space=pltpu.SMEM)


def forward(me, geo, entry, counts, tgt, w_in, w_mid, w_out, b_hid, b_out, freqs, delta):
    res = [jax.ShapeDtypeStruct((32 * ROWS, 128), F32), pltpu.VMEM((SAMP, 8, RAYS), F32)]
    res += [pltpu.VMEM((SAMP, H, RAYS), BF16)] * 8 + [pltpu.VMEM((SAMP, H, RAYS), F32)] * 3
    return pl.pallas_call(
        lambda *refs: forward_kernel(*refs, delta=delta),
        grid=(STEPS,),
        in_specs=[smem()] + [full(x.shape) for x in (geo, entry, counts, tgt, w_in, w_mid, w_out, b_hid, b_out, freqs)],
        out_specs=[full((32 * ROWS, 128)), vmem()] + [vmem()] * 11,
        out_shape=res,
        scratch_shapes=[
            pltpu.VMEM((3, H, 3 * H), BF16), pltpu.VMEM((16, H), BF16),
            pltpu.VMEM((3, H, 128), F32), pltpu.VMEM((H, RAYS), F32), pltpu.VMEM((H, RAYS), F32),
            pltpu.VMEM((1, RAYS), F32), pltpu.VMEM((8, RAYS), F32),
        ],
        compiler_params=pltpu.CompilerParams(vmem_limit_bytes=28 * 1024 * 1024),
        name="fwd",
    )(me, geo, entry, counts, tgt, w_in, w_mid, w_out, b_hid, b_out, freqs)


def backward_kernel(
    me_ref, recv_ref, counts_ref, win_ref, wmid_ref, wout_ref, out_ref,
    fh_ref, fl_ref, h1h_ref, h1l_ref, h2h_ref, h2l_ref, h3h_ref, h3l_ref, s1_ref, s2_ref, s3_ref,
    pix_ref, mine_ref, other_ref,
    wcat, wo, g_all, adj, pixs, acc, bacc, gacc, goacc, dh_buf,
    *, delta, factor,
):
    step = pl.program_id(0)

    @pl.when(step == 0)
    def _():
        me = me_ref[0]
        for i in range(2):
            hi, lo = split(wmid_ref[0, i])
            wcat[i, :, 0:256] = hi
            wcat[i, :, 256:512] = hi
            wcat[i, :, 512:768] = lo
        w8 = jnp.concatenate([wout_ref[0], jnp.zeros((4, H), F32)], axis=0)
        hi, lo = split(w8)
        hi, lo = hi.astype(F32), lo.astype(F32)
        wo[...] = jnp.concatenate([hi, hi, lo, jnp.zeros((104, H), F32)], axis=0).T[:, 0:32].astype(BF16)
        acc[...] = jnp.zeros_like(acc)
        bacc[...] = jnp.zeros_like(bacc)
        gacc[...] = jnp.zeros_like(gacc)
        goacc[...] = jnp.zeros_like(goacc)
        zero = jnp.zeros((4, 128), F32)
        depth, own, pix, after = zero, zero, [zero] * 3, [zero] * 3
        for s in range(32):
            shade = jnp.exp(depth)
            own = jnp.where(me == s, shade, own)
            late = jnp.where(s > me, F32(1.0), F32(0.0))
            for c in range(3):
                part = shade * recv_ref[s * ROWS + 4 * c : s * ROWS + 4 * c + 4]
                pix[c] = pix[c] + part
                after[c] = after[c] + late * part
            depth = depth + recv_ref[s * ROWS + 12 : s * ROWS + 16]
        through = jnp.exp(depth)
        lane = lax.broadcasted_iota(jnp.int32, (8, 128), 1)
        sub = lax.broadcasted_iota(jnp.int32, (8, 128), 0)
        adj[...] = jnp.zeros_like(adj)
        log_adj = zero
        for c in range(3):
            rows = []
            for q in range(4):
                t = jnp.concatenate(
                    [recv_ref[(8 * q + s) * ROWS + 16 : (8 * q + s) * ROWS + 17] for s in range(8)], axis=0
                )
                if c:
                    t = pltpu.roll(t, 128 - OWN * c, 1)
                t = jnp.where(lax.div(lane, OWN) == sub, t, F32(0.0))
                rows.append(jnp.sum(t, axis=0, keepdims=True))
            target = jnp.concatenate(rows, axis=0)
            pixel = pix[c] + through
            pixs[4 * c : 4 * c + 4] = pixel
            dpix = F32(2.0 * factor) * (pixel - target)
            log_adj = log_adj + dpix * (after[c] + through)
            a = own * dpix
            for q in range(4):
                adj[c + 1 : c + 2, 128 * q : 128 * q + 128] = a[q : q + 1]
        for c in range(3):
            row = pixs[pl.ds(4 * c + lax.div(me, 8), 1), :]
            row = pltpu.roll(jnp.broadcast_to(row, (8, 128)), lax.rem(128 - lax.rem(me, 8) * OWN, 128), 1)
            pix_ref[c] = row[0:1, 0:OWN]
        log_adj = jnp.concatenate([log_adj[q : q + 1] for q in range(4)], axis=1)
        a8 = adj[...]
        counts = counts_ref[0]
        bef = jnp.zeros((1, RAYS), F32)
        ends, weights = [], []
        for j in range(SAMP):
            dep = jnp.where(j < counts, softplus(out_ref[j, 0:1]) * F32(delta), F32(0.0))
            weights.append(jnp.exp(-bef) * (F32(1.0) - jnp.exp(-dep)))
            bef = bef + dep
            ends.append(jnp.exp(-bef))
        later = jnp.zeros((8, RAYS), F32)
        first = lax.broadcasted_iota(jnp.int32, (8, RAYS), 0) == 0
        for j in reversed(range(SAMP)):
            sg = sigmoid(out_ref[j])
            ddep = jnp.sum(a8 * (ends[j] * sg - later), axis=0, keepdims=True) - log_adj
            ddep = jnp.where(j < counts, F32(delta) * ddep, F32(0.0))
            g = jnp.where(first, ddep * sg, a8 * weights[j] * (sg * (F32(1.0) - sg)))
            later = later + weights[j] * sg
            g_all[j] = g

    n = step * SPB
    for j in range(SPB):
        g = g_all[step * SPB + j]
        gacc[...] += g[:, 0:128] + g[:, 128:256] + g[:, 256:384] + g[:, 384:512]
        gb = [[jnp.broadcast_to(g[c : c + 1, 128 * t : 128 * t + 128], (8, 128)) for t in range(4)] for c in range(4)]
        for r in range(0, H, 16):
            rows = slice(r, r + 16)
            parts = [None] * 4
            for t in range(4):
                lanes = slice(128 * t, 128 * t + 128)
                h3 = h3h_ref[n + j, rows, lanes].astype(F32) + h3l_ref[n + j, rows, lanes].astype(F32)
                for c in range(4):
                    p = jnp.concatenate([h3[0:8] * gb[c][t], h3[8:16] * gb[c][t]], axis=0)
                    parts[c] = p if parts[c] is None else parts[c] + p
            for c in range(4):
                goacc[c, rows] += parts[c]
        gh, gl = split(g)
        gh, gl = gh.astype(F32), gl.astype(F32)
        gk = jnp.concatenate([gh, gl, gh, jnp.zeros((8, RAYS), F32)], axis=0).astype(BF16)
        dh_buf[j] = mm(wo[...], gk)
    sigs = (s3_ref, s2_ref, s1_ref)
    hs = ((h2h_ref, h2l_ref), (h1h_ref, h1l_ref), (fh_ref, fl_ref))
    for i in range(3):
        lhs, rhs = [], []
        for j in range(SPB):
            dx = dh_buf[j] * sigs[i][n + j]
            bacc[2 - i] += dx[:, 0:128] + dx[:, 128:256] + dx[:, 256:384] + dx[:, 384:512]
            xh, xl = split(dx)
            lhs += [hs[i][0][n + j], hs[i][0][n + j], hs[i][1][n + j]]
            rhs += [xh, xl, xh]
            if i < 2:
                dh_buf[j] = mm(wcat[1 - i], jnp.concatenate([xh, xl, xh], axis=0))
        acc[2 - i] += mm_nt(jnp.concatenate(lhs, axis=1), jnp.concatenate(rhs, axis=1))

    @pl.when(step == STEPS - 1)
    def _():
        core, chip = me_ref[1], me_ref[2]
        for k in range(4):
            q = lax.rem(chip + k, 4)
            for i in range(3):
                rows = pl.ds(96 * k + 32 * i, 32)
                unit = F32(LN2 if i else 1.0)
                mine_ref[rows] = acc[i, pl.ds((core * 4 + q) * 32, 32), :] * unit
                other_ref[rows] = acc[i, pl.ds(((1 - core) * 4 + q) * 32, 32), :] * unit
        lane = lax.broadcasted_iota(jnp.int32, (8, 128), 1)
        sub = lax.broadcasted_iota(jnp.int32, (8, 128), 0)
        hid = [jnp.sum(bacc[i].T, axis=0, keepdims=True) for i in range(3)]
        gb = jnp.broadcast_to(jnp.sum(gacc[...], axis=1, keepdims=True), (8, 128))
        gb = jnp.sum(jnp.where(lane == sub, gb, F32(0.0)), axis=0, keepdims=True)
        gb = jnp.concatenate([gb, jnp.zeros((1, 128), F32)], axis=1)
        outw = [jnp.sum(goacc[c].T, axis=0, keepdims=True) * F32(LN2) for c in range(4)]
        small = jnp.concatenate(outw + hid + [gb], axis=0)
        mine_ref[384:392] = small
        other_ref[384:392] = small


def backward(ids, recv, counts, w_in, w_mid, w_out, out, residuals, delta, factor):
    half = pltpu.VMEM((392, H), F32)
    recv, out = keep(recv), keep(out)
    residuals = [keep(x) for x in residuals]
    return pl.pallas_call(
        lambda *refs: backward_kernel(*refs, delta=delta, factor=factor),
        grid=(STEPS,),
        in_specs=[smem(), vmem()] + [full(x.shape) for x in (counts, w_in, w_mid, w_out)] + [vmem()] + [vmem()] * 11,
        out_specs=[full((3, 1, OWN)), vmem(), vmem()],
        out_shape=[jax.ShapeDtypeStruct((3, 1, OWN), F32), half, half],
        scratch_shapes=[
            pltpu.VMEM((2, H, 3 * H), BF16), pltpu.VMEM((H, 32), BF16),
            pltpu.VMEM((SAMP, 8, RAYS), F32), pltpu.VMEM((8, RAYS), F32), pltpu.VMEM((16, 128), F32),
            pltpu.VMEM((3, H, H), F32), pltpu.VMEM((3, H, 128), F32), pltpu.VMEM((8, 128), F32), pltpu.VMEM((4, H, 128), F32),
            pltpu.VMEM((SPB, H, RAYS), F32),
        ],
        compiler_params=pltpu.CompilerParams(vmem_limit_bytes=28 * 1024 * 1024),
        name="bwd",
    )(ids, recv, counts, w_in, w_mid, w_out, out, *residuals)


def place_kernel(ids_ref, done, own1, own2, own3, sib, gin, gmid, gout, ghid, gbout):
    own = (done, own1, own2, own3)
    core, chip = ids_ref[1], ids_ref[2]
    for k in range(4):
        q = lax.rem(chip + 4 - k, 4)
        for side in range(2):
            src, base = (own[k], 0) if side == 0 else (sib, 96 * k)
            rows = pl.ds(((core if side == 0 else 1 - core) * 4 + q) * 32, 32)
            gin[0, rows] = src[base : base + 32]
            gmid[0, 0, rows] = src[base + 32 : base + 64]
            gmid[0, 1, rows] = src[base + 64 : base + 96]
    gout[0] = done[96:100]
    for i in range(3):
        ghid[i] = done[100 + i : 101 + i]
    gbout[...] = done[103:104, 0:4]


def place(ids, done, own, sib):
    shapes = [(1, H, H), (1, 2, H, H), (1, 4, H), (3, 1, H), (1, 4)]
    return pl.pallas_call(
        place_kernel,
        in_specs=[smem()] + [vmem()] * 5,
        out_specs=[vmem()] * 5,
        out_shape=[jax.ShapeDtypeStruct(x, F32) for x in shapes],
        compiler_params=pltpu.CompilerParams(vmem_limit_bytes=16 * 1024 * 1024),
        name="place",
    )(ids, *[keep(x) for x in (done, *own, sib)])


def shards(geometry, entry, counts, targets, w_in, w_mid, w_out, b_hid, b_out, freqs):
    slabs = lax.axis_size("slab")
    delta = 3.0 / (SAMP * slabs)
    factor = 1.0 / math.sqrt(3.0 * lax.axis_size("rays") * slabs * OWN)
    me = lax.axis_index("slab")
    ray = lax.axis_index("rays")
    ids = jnp.stack([me, lax.rem(ray, 2), lax.div(ray, 2)]).astype(jnp.int32)
    send, out, *residuals = forward(
        ids, geometry, entry, counts, targets, w_in, w_mid, w_out,
        b_hid.transpose(1, 0, 2), b_out, freqs.transpose(1, 0, 2), delta
    )
    recv = lax.all_to_all(send.reshape(32, 1, ROWS * 128), "slab", 0, 0, tiled=True).reshape(32 * ROWS, 128)
    pixels, mine, other = backward(ids, recv, counts, w_in, w_mid, w_out, out, residuals, delta, factor)
    swap = [(i, i ^ 1) for i in range(8)]
    along = [[(i, (i + 2 * k) % 8) for i in range(8)] for k in range(4)]
    total = mine + lax.ppermute(other, "rays", swap)
    small = total[384:392]
    parts = [jnp.concatenate([total[96 * k : 96 * k + 96], small], axis=0) for k in range(4)]
    got = [lax.ppermute(parts[k], "rays", along[k]) for k in range(1, 4)]
    done = parts[0] + got[0] + got[1] + got[2]
    chunk = done[0:96]
    own = [lax.ppermute(chunk, "rays", along[k]) for k in range(1, 4)]
    sib = lax.ppermute(jnp.concatenate([chunk] + own, axis=0), "rays", swap)
    grad_in, grad_mid, grad_out, grad_hid, grad_bout = place(ids, done, own, sib)
    return pixels, grad_in, grad_mid, grad_out, grad_hid.transpose(1, 0, 2), grad_bout


def solution(mesh):
    in_specs = (
        P(None, "rays", None),
        P("slab", "rays", None),
        P("slab", "rays", None),
        P(None, "rays", "slab"),
        P("slab", None, None),
        P("slab", None, None, None),
        P("slab", None, None),
        P("slab", None, None),
        P("slab", None),
        P("slab", None, None),
    )
    out_specs = (
        P(None, "rays", "slab"),
        P("slab", None, None),
        P("slab", None, None, None),
        P("slab", None, None),
        P("slab", None, None),
        P("slab", None),
    )
    return jax.shard_map(shards, mesh=mesh, in_specs=in_specs, out_specs=out_specs, check_vma=False)
```

```python
import math

import jax
import jax.numpy as jnp
from jax import lax
from jax.experimental import pallas as pl
from jax.experimental.pallas import tpu as pltpu
from jax.sharding import PartitionSpec as P

H = 256
FE = 128
SAMP = 8
RAYS = 512
OWN = 16
ROWS = 17
SF = 8
SB = 8
NF = SAMP // SF
NB = SAMP // SB
F32 = jnp.float32
LOG2E = 1.4426950408889634
LN2 = 0.6931471805599453
BF16 = jnp.bfloat16
NT = (((1,), (1,)), ((), ()))


def mm(a, b):
    return jnp.dot(a, b, preferred_element_type=F32)


def mm_nt(a, b):
    return lax.dot_general(a, b, NT, preferred_element_type=F32)


def split(x):
    hi = x.astype(BF16)
    return hi, (x - hi.astype(F32)).astype(BF16)


def sincos(phase):
    turns = jnp.floor(phase * F32(2.0 / math.pi) + F32(0.5))
    r = phase - turns * F32(1.5703125)
    r = r - turns * F32(math.pi / 2 - 1.5703125)
    z = r * r
    s = r + r * z * (F32(-1.6666654611e-1) + z * (F32(8.3321608736e-3) + z * F32(-1.9515295891e-4)))
    c = F32(1.0) - F32(0.5) * z + z * z * (
        F32(4.166664568298827e-2) + z * (F32(-1.388731625493765e-3) + z * F32(2.443315711809948e-5))
    )
    k = turns.astype(jnp.int32)
    odd = (k & 1) == 1
    sine = jnp.where(odd, c, s)
    cosine = jnp.where(odd, s, c)
    sine = jnp.where((k & 2) == 2, -sine, sine)
    cosine = jnp.where(((k + 1) & 2) == 2, -cosine, cosine)
    return sine, cosine


def softplus(x):
    u = jnp.exp(-jnp.abs(x))
    w = F32(1.0) + u
    return jnp.maximum(x, F32(0.0)) + (jnp.log(w) + (u - (w - F32(1.0))))


def softplus2(x):
    v = jnp.exp2(jnp.minimum(x, F32(100.0)))
    log = lax.log2(F32(1.0 + 2.0**-23) + v)
    return jnp.maximum(jnp.minimum(log, v * F32(LOG2E)), x)


def sigmoid(x):
    u = jnp.exp(-jnp.abs(x))
    return jnp.where(x >= 0, F32(1.0), u) / (F32(1.0) + u)


def forward_kernel(
    geo_ref, entry_ref, counts_ref, tgt_ref, win_ref, wmid_ref, wout_ref, bhid_ref, bout_ref, freqs_ref,
    send_ref, wb_ref, wob_ref, out_ref, fh_ref, fl_ref, h1h_ref, h1l_ref, h2h_ref, h2l_ref, h3h_ref, h3l_ref, s1_ref, s2_ref, s3_ref,
    wcat, wo, bias, rot, feat, before, color,
    *, delta,
):
    step = pl.program_id(0)

    @pl.when(step == 0)
    def _():
        for i in range(3):
            w = win_ref[0] * F32(LOG2E) if i == 0 else wmid_ref[0, i - 1]
            hi, lo = split(w.T)
            wcat[i, :, 0:256] = hi
            wcat[i, :, 256:512] = hi
            wcat[i, :, 512:768] = lo
            bias[i] = jnp.broadcast_to(bhid_ref[i] * F32(LOG2E), (128, H)).T
        w8 = jnp.concatenate([wout_ref[0] * F32(LN2), jnp.zeros((4, H), F32)], axis=0)
        hi, lo = split(w8)
        wo[...] = jnp.concatenate([hi.astype(F32), lo.astype(F32)], axis=0).astype(BF16)
        for i in range(2):
            hi, lo = split(wmid_ref[0, i])
            wb_ref[i, :, 0:256] = hi
            wb_ref[i, :, 256:512] = hi
            wb_ref[i, :, 512:768] = lo
        w8 = jnp.concatenate([wout_ref[0], jnp.zeros((4, H), F32)], axis=0)
        hi, lo = split(w8)
        hi, lo = hi.astype(F32), lo.astype(F32)
        wob_ref[...] = jnp.concatenate([hi, hi, lo, jnp.zeros((104, H), F32)], axis=0).T[:, 0:32].astype(BF16)
        ft = jnp.concatenate([freqs_ref[0], freqs_ref[1], freqs_ref[2], jnp.zeros((5, FE), F32)], axis=0).T
        geo = geo_ref[:, 0, :]
        a = ft[:, 0:1] * geo[0:1] + ft[:, 1:2] * geo[1:2] + ft[:, 2:3] * geo[2:3]
        d = ft[:, 0:1] * geo[3:4] + ft[:, 1:2] * geo[4:5] + ft[:, 2:3] * geo[5:6]
        t0 = F32(0.25) * (entry_ref[0].astype(F32) + F32(0.5))
        s, c = sincos(a + t0 * d)
        feat[0:FE] = s
        feat[FE:] = c
        s, c = sincos(F32(0.25) * d)
        rot[0:FE] = s
        rot[FE:] = c
        before[...] = jnp.zeros_like(before)
        color[...] = jnp.zeros_like(color)

    n = step * SF

    def slot_input(j):
        s, c = feat[0:FE], feat[FE:]
        fh_ref[n + j, 0:FE], fl_ref[n + j, 0:FE] = split(s)
        fh_ref[n + j, FE:], fl_ref[n + j, FE:] = split(c)
        rs, rc = rot[0:FE], rot[FE:]
        feat[0:FE] = s * rc + c * rs
        feat[FE:] = c * rc - s * rs

    for j in range(SF):
        slot_input(j)
    srcs = [(fh_ref, fl_ref), (h1h_ref, h1l_ref), (h2h_ref, h2l_ref), (h3h_ref, h3l_ref)]
    sigs = [s1_ref, s2_ref, s3_ref]
    parts = [(j, k) for j in range(SF) for k in range(2)]
    for i in range(3):
        b = jnp.concatenate([bias[i], bias[i]], axis=1)
        for j, k in parts:
            lanes = slice(256 * k, 256 * k + 256)
            hi = srcs[i][0][n + j, :, lanes]
            lo = srcs[i][1][n + j, :, lanes]
            x = mm(wcat[i], jnp.concatenate([hi, lo, hi], axis=0)) + b
            h = softplus2(x)
            sigs[i][n + j, :, lanes] = jnp.exp2(x - h)
            srcs[i + 1][0][n + j, :, lanes], srcs[i + 1][1][n + j, :, lanes] = split(h)
    bo = jnp.concatenate([bout_ref[0:1, :], jnp.zeros((1, 124), F32)], axis=1)
    bo = jnp.broadcast_to(bo, (128, 128)).T[0:8, 0:1]
    for j in range(SF):
        d1 = mm(wo[...], h3h_ref[n + j])
        d2 = mm(wo[...], h3l_ref[n + j])
        o = d1[0:8] + d1[8:16] + d2[0:8] + d2[8:16] + bo
        gate = jnp.where(step * SF + j < counts_ref[0], F32(delta), F32(0.0))
        depth = softplus(o[0:1]) * gate
        bef = before[...]
        w = jnp.exp(-bef) * (F32(1.0) - jnp.exp(-depth))
        sg = sigmoid(o)
        color[...] += w * sg
        before[...] = bef + depth
        out_ref[step * SF + j] = jnp.concatenate([sg[0:4], w, jnp.exp(-(bef + depth)), gate, jnp.zeros_like(w)], axis=0)

    @pl.when(step == NF - 1)
    def _():
        t = tgt_ref[:, 0, :]
        t = jnp.concatenate([t[0:1], t[1:2], t[2:3], jnp.zeros((1, 80), F32)], axis=1)
        t = pltpu.roll(jnp.broadcast_to(t, (8, 128)), lax.rem(lax.axis_index("slab"), 8) * OWN, 1)[0:1]
        rows = []
        for c in range(4):
            v = color[c + 1 : c + 2] if c < 3 else -before[...]
            rows += [v[:, 128 * q : 128 * q + 128] for q in range(4)]
        rows.append(t)
        value = jnp.concatenate(rows, axis=0)
        for s in range(32):
            send_ref[s * ROWS : (s + 1) * ROWS] = value


def where():
    ray = lax.axis_index("rays")
    return lax.rem(ray, 2), lax.div(ray, 2)


def keep(x):
    return pltpu.with_memory_space_constraint(x, pltpu.VMEM)


def vmem():
    return pl.BlockSpec(memory_space=pltpu.VMEM)


def full(shape):
    return pl.BlockSpec(shape, lambda i, n=len(shape): (0,) * n)


def forward(geo, entry, counts, tgt, w_in, w_mid, w_out, b_hid, b_out, freqs, delta):
    res = [jax.ShapeDtypeStruct((32 * ROWS, 128), F32), pltpu.VMEM((2, H, 3 * H), BF16), pltpu.VMEM((H, 32), BF16), pltpu.VMEM((SAMP, 8, RAYS), F32)]
    res += [pltpu.VMEM((SAMP, H, RAYS), BF16)] * 8 + [pltpu.VMEM((SAMP, H, RAYS), F32)] * 3
    return pl.pallas_call(
        lambda *refs: forward_kernel(*refs, delta=delta),
        grid=(NF,),
        in_specs=[full(x.shape) for x in (geo, entry, counts, tgt, w_in, w_mid, w_out, b_hid, b_out, freqs)],
        out_specs=[full((32 * ROWS, 128))] + [vmem()] * 14,
        out_shape=res,
        scratch_shapes=[
            pltpu.VMEM((3, H, 3 * H), BF16), pltpu.VMEM((16, H), BF16),
            pltpu.VMEM((3, H, 128), F32), pltpu.VMEM((H, RAYS), F32), pltpu.VMEM((H, RAYS), F32),
            pltpu.VMEM((1, RAYS), F32), pltpu.VMEM((8, RAYS), F32),
        ],
        compiler_params=pltpu.CompilerParams(vmem_limit_bytes=28 * 1024 * 1024),
        name="fwd",
    )(geo, entry, counts, tgt, w_in, w_mid, w_out, b_hid, b_out, freqs)


def backward_kernel(
    recv_ref, wcat, wo, out_ref,
    fh_ref, fl_ref, h1h_ref, h1l_ref, h2h_ref, h2l_ref, h3h_ref, h3l_ref, s1_ref, s2_ref, s3_ref,
    pix_ref, mine_ref, other_ref,
    g_all, adj, pixs, acc, bacc, gacc, goacc, dh_buf,
    *, factor,
):
    step = pl.program_id(0)

    @pl.when(step == 0)
    def _():
        me = lax.axis_index("slab")
        acc[...] = jnp.zeros_like(acc)
        bacc[...] = jnp.zeros_like(bacc)
        gacc[...] = jnp.zeros_like(gacc)
        goacc[...] = jnp.zeros_like(goacc)
        zero = jnp.zeros((4, 128), F32)
        depth, own, pix, after = zero, zero, [zero] * 3, [zero] * 3
        for s in range(32):
            shade = jnp.exp(depth)
            own = jnp.where(me == s, shade, own)
            late = jnp.where(s > me, F32(1.0), F32(0.0))
            for c in range(3):
                part = shade * recv_ref[s * ROWS + 4 * c : s * ROWS + 4 * c + 4]
                pix[c] = pix[c] + part
                after[c] = after[c] + late * part
            depth = depth + recv_ref[s * ROWS + 12 : s * ROWS + 16]
        through = jnp.exp(depth)
        lane = lax.broadcasted_iota(jnp.int32, (8, 128), 1)
        sub = lax.broadcasted_iota(jnp.int32, (8, 128), 0)
        adj[...] = jnp.zeros_like(adj)
        log_adj = zero
        for c in range(3):
            rows = []
            for q in range(4):
                t = jnp.concatenate(
                    [recv_ref[(8 * q + s) * ROWS + 16 : (8 * q + s) * ROWS + 17] for s in range(8)], axis=0
                )
                if c:
                    t = pltpu.roll(t, 128 - OWN * c, 1)
                t = jnp.where(lax.div(lane, OWN) == sub, t, F32(0.0))
                rows.append(jnp.sum(t, axis=0, keepdims=True))
            target = jnp.concatenate(rows, axis=0)
            pixel = pix[c] + through
            pixs[4 * c : 4 * c + 4] = pixel
            dpix = F32(2.0 * factor) * (pixel - target)
            log_adj = log_adj + dpix * (after[c] + through)
            a = own * dpix
            for q in range(4):
                adj[c + 1 : c + 2, 128 * q : 128 * q + 128] = a[q : q + 1]
        for c in range(3):
            row = pixs[pl.ds(4 * c + lax.div(me, 8), 1), :]
            row = pltpu.roll(jnp.broadcast_to(row, (8, 128)), lax.rem(128 - lax.rem(me, 8) * OWN, 128), 1)
            pix_ref[c] = row[0:1, 0:OWN]
        log_adj = jnp.concatenate([log_adj[q : q + 1] for q in range(4)], axis=1)
        a8 = adj[...]
        later = jnp.zeros((8, RAYS), F32)
        first = lax.broadcasted_iota(jnp.int32, (8, RAYS), 0) == 0
        for j in reversed(range(SAMP)):
            sg = out_ref[j]
            w, end, gate = sg[4:5], sg[5:6], sg[6:7]
            ddep = gate * (jnp.sum(a8 * (end * sg - later), axis=0, keepdims=True) - log_adj)
            g = jnp.where(first, ddep * sg, a8 * w * (sg * (F32(1.0) - sg)))
            later = later + w * sg
            g_all[j] = g

    n = step * SB
    for j in range(SB):
        g = g_all[step * SB + j]
        gacc[...] += g[:, 0:128] + g[:, 128:256] + g[:, 256:384] + g[:, 384:512]
        gb = [[jnp.broadcast_to(g[c : c + 1, 128 * t : 128 * t + 128], (8, 128)) for t in range(4)] for c in range(4)]
        for r in range(0, H, 16):
            rows = slice(r, r + 16)
            parts = [None] * 4
            for t in range(4):
                lanes = slice(128 * t, 128 * t + 128)
                h3 = h3h_ref[n + j, rows, lanes].astype(F32) + h3l_ref[n + j, rows, lanes].astype(F32)
                for c in range(4):
                    p = jnp.concatenate([h3[0:8] * gb[c][t], h3[8:16] * gb[c][t]], axis=0)
                    parts[c] = p if parts[c] is None else parts[c] + p
            for c in range(4):
                goacc[c, rows] += parts[c]
        gh, gl = split(g)
        gh, gl = gh.astype(F32), gl.astype(F32)
        gk = jnp.concatenate([gh, gl, gh, jnp.zeros((8, RAYS), F32)], axis=0).astype(BF16)
        dh_buf[j] = mm(wo[...], gk)
    sigs = (s3_ref, s2_ref, s1_ref)
    hs = ((h2h_ref, h2l_ref), (h1h_ref, h1l_ref), (fh_ref, fl_ref))
    for i in range(3):
        lhs, rhs = [], []
        for j in range(SB):
            dx = dh_buf[j] * sigs[i][n + j]
            bacc[2 - i] += dx[:, 0:128] + dx[:, 128:256] + dx[:, 256:384] + dx[:, 384:512]
            xh, xl = split(dx)
            lhs += [hs[i][0][n + j], hs[i][0][n + j], hs[i][1][n + j]]
            rhs += [xh, xl, xh]
            if i < 2:
                dh_buf[j] = mm(wcat[1 - i], jnp.concatenate([xh, xl, xh], axis=0))
        acc[2 - i] += mm_nt(jnp.concatenate(lhs, axis=1), jnp.concatenate(rhs, axis=1))

    @pl.when(step == NB - 1)
    def _():
        core, chip = where()
        for k in range(4):
            q = lax.rem(chip + k, 4)
            for i in range(3):
                rows = pl.ds(96 * k + 32 * i, 32)
                unit = F32(LN2 if i else 1.0)
                mine_ref[rows] = acc[i, pl.ds((core * 4 + q) * 32, 32), :] * unit
                other_ref[rows] = acc[i, pl.ds(((1 - core) * 4 + q) * 32, 32), :] * unit
        lane = lax.broadcasted_iota(jnp.int32, (8, 128), 1)
        sub = lax.broadcasted_iota(jnp.int32, (8, 128), 0)
        hid = [jnp.sum(bacc[i].T, axis=0, keepdims=True) for i in range(3)]
        gb = jnp.broadcast_to(jnp.sum(gacc[...], axis=1, keepdims=True), (8, 128))
        gb = jnp.sum(jnp.where(lane == sub, gb, F32(0.0)), axis=0, keepdims=True)
        gb = jnp.concatenate([gb, jnp.zeros((1, 128), F32)], axis=1)
        outw = [jnp.sum(goacc[c].T, axis=0, keepdims=True) * F32(LN2) for c in range(4)]
        small = jnp.concatenate(outw + hid + [gb], axis=0)
        mine_ref[384:392] = small
        other_ref[384:392] = small


def backward(recv, wb, wo, out, residuals, factor):
    args = [keep(x) for x in (recv, wb, wo, out, *residuals)]
    return pl.pallas_call(
        lambda *refs: backward_kernel(*refs, factor=factor),
        grid=(NB,),
        in_specs=[vmem()] * len(args),
        out_specs=[vmem()] * 3,
        out_shape=[pltpu.VMEM((3, 1, OWN), F32), pltpu.VMEM((392, H), F32), pltpu.VMEM((392, H), F32)],
        scratch_shapes=[
            pltpu.VMEM((SAMP, 8, RAYS), F32), pltpu.VMEM((8, RAYS), F32), pltpu.VMEM((16, 128), F32),
            pltpu.VMEM((3, H, H), F32), pltpu.VMEM((3, H, 128), F32), pltpu.VMEM((8, 128), F32), pltpu.VMEM((4, H, 128), F32),
            pltpu.VMEM((SB, H, RAYS), F32),
        ],
        compiler_params=pltpu.CompilerParams(vmem_limit_bytes=24 * 1024 * 1024),
        name="bwd",
    )(*args)


def copies(side, sources, gin, gmid, sem):
    core, chip = where()
    started = []
    for k in range(4):
        q = lax.rem(chip + 4 - k, 4)
        rows = pl.ds(((core if side == 0 else 1 - core) * 4 + q) * 32, 32)
        src, base = sources(k)
        for i, dst in enumerate((gin.at[0, rows], gmid.at[0, 0, rows], gmid.at[0, 1, rows])):
            copy = pltpu.make_async_copy(src.at[pl.ds(base + 32 * i, 32)], dst, sem.at[3 * k + i])
            copy.start()
            started.append(copy)
    return started


def place_own_kernel(done, own1, own2, own3, gin, gmid, gout, ghid, gbout, sem):
    own = (done, own1, own2, own3)
    started = copies(0, lambda k: (own[k], 0), gin, gmid, sem)
    gout[0] = done[96:100]
    for i in range(3):
        ghid[i] = done[100 + i : 101 + i]
    gbout[...] = done[103:104, 0:4]
    for copy in started:
        copy.wait()


def place_other_kernel(sib, gin_in, gmid_in, gin, gmid, sem):
    for copy in copies(1, lambda k: (sib, 96 * k), gin, gmid, sem):
        copy.wait()


def hbm():
    return pl.BlockSpec(memory_space=pl.ANY)


def place_own(done, own):
    shapes = [(1, H, H), (1, 2, H, H), (1, 4, H), (3, 1, H), (1, 4)]
    return pl.pallas_call(
        place_own_kernel,
        in_specs=[vmem()] * 4,
        out_specs=[hbm()] * 2 + [vmem()] * 3,
        out_shape=[jax.ShapeDtypeStruct(x, F32) for x in shapes],
        scratch_shapes=[pltpu.SemaphoreType.DMA((12,))],
        compiler_params=pltpu.CompilerParams(vmem_limit_bytes=16 * 1024 * 1024),
        name="place_own",
    )(*[keep(x) for x in (done, *own)])


def place_other(sib, gin, gmid):
    return pl.pallas_call(
        place_other_kernel,
        in_specs=[vmem()] + [hbm()] * 2,
        out_specs=[hbm()] * 2,
        out_shape=[jax.ShapeDtypeStruct(x.shape, F32) for x in (gin, gmid)],
        scratch_shapes=[pltpu.SemaphoreType.DMA((12,))],
        input_output_aliases={1: 0, 2: 1},
        compiler_params=pltpu.CompilerParams(vmem_limit_bytes=16 * 1024 * 1024),
        name="place_other",
    )(keep(sib), gin, gmid)


def shards(geometry, entry, counts, targets, w_in, w_mid, w_out, b_hid, b_out, freqs):
    slabs = lax.axis_size("slab")
    delta = 3.0 / (SAMP * slabs)
    factor = 1.0 / math.sqrt(3.0 * lax.axis_size("rays") * slabs * OWN)
    send, wb, wo, out, *residuals = forward(
        geometry, entry, counts, targets, w_in, w_mid, w_out,
        b_hid.transpose(1, 0, 2), b_out, freqs.transpose(1, 0, 2), delta
    )
    recv = lax.all_to_all(send.reshape(32, 1, ROWS * 128), "slab", 0, 0, tiled=True).reshape(32 * ROWS, 128)
    pixels, mine, other = backward(recv, wb, wo, out, residuals, factor)
    swap = [(i, i ^ 1) for i in range(8)]
    along = [[(i, (i + 2 * k) % 8) for i in range(8)] for k in range(4)]
    total = mine + lax.ppermute(other, "rays", swap)
    small = total[384:392]
    parts = [jnp.concatenate([total[96 * k : 96 * k + 96], small], axis=0) for k in range(4)]
    got = [lax.ppermute(parts[k], "rays", along[k]) for k in range(1, 4)]
    done = parts[0] + got[0] + got[1] + got[2]
    chunk = done[0:96]
    own = [lax.ppermute(chunk, "rays", along[k]) for k in range(1, 4)]
    sib = lax.ppermute(jnp.concatenate([chunk] + own, axis=0), "rays", swap)
    grad_in, grad_mid, grad_out, grad_hid, grad_bout = place_own(done, own)
    grad_in, grad_mid = place_other(sib, grad_in, grad_mid)
    return pixels, grad_in, grad_mid, grad_out, grad_hid.transpose(1, 0, 2), grad_bout


def solution(mesh):
    in_specs = (
        P(None, "rays", None),
        P("slab", "rays", None),
        P("slab", "rays", None),
        P(None, "rays", "slab"),
        P("slab", None, None),
        P("slab", None, None, None),
        P("slab", None, None),
        P("slab", None, None),
        P("slab", None),
        P("slab", None, None),
    )
    out_specs = (
        P(None, "rays", "slab"),
        P("slab", None, None),
        P("slab", None, None, None),
        P("slab", None, None),
        P("slab", None, None),
        P("slab", None),
    )
    return jax.shard_map(shards, mesh=mesh, in_specs=in_specs, out_specs=out_specs, check_vma=False)
```

```python
import math

import jax
import jax.numpy as jnp
from jax import lax
from jax.experimental import pallas as pl
from jax.experimental.pallas import tpu as pltpu
from jax.sharding import PartitionSpec as P

H = 256
FE = 128
SAMP = 8
RAYS = 512
OWN = 16
ROWS = 17
SF = 8
SB = 8
NF = SAMP // SF
NB = SAMP // SB
ORDER = (0, 3, 1, 2)
F32 = jnp.float32
LOG2E = 1.4426950408889634
LN2 = 0.6931471805599453
BF16 = jnp.bfloat16
NT = (((1,), (1,)), ((), ()))


def mm(a, b):
    return jnp.dot(a, b, preferred_element_type=F32)


def mm_nt(a, b):
    return lax.dot_general(a, b, NT, preferred_element_type=F32)


def split(x):
    hi = x.astype(BF16)
    return hi, (x - hi.astype(F32)).astype(BF16)


def sincos(phase):
    turns = jnp.floor(phase * F32(2.0 / math.pi) + F32(0.5))
    r = phase - turns * F32(1.5703125)
    r = r - turns * F32(math.pi / 2 - 1.5703125)
    z = r * r
    s = r + r * z * (F32(-1.6666654611e-1) + z * (F32(8.3321608736e-3) + z * F32(-1.9515295891e-4)))
    c = F32(1.0) - F32(0.5) * z + z * z * (
        F32(4.166664568298827e-2) + z * (F32(-1.388731625493765e-3) + z * F32(2.443315711809948e-5))
    )
    k = turns.astype(jnp.int32)
    odd = (k & 1) == 1
    sine = jnp.where(odd, c, s)
    cosine = jnp.where(odd, s, c)
    sine = jnp.where((k & 2) == 2, -sine, sine)
    cosine = jnp.where(((k + 1) & 2) == 2, -cosine, cosine)
    return sine, cosine


def softplus(x):
    u = jnp.exp(-jnp.abs(x))
    w = F32(1.0) + u
    return jnp.maximum(x, F32(0.0)) + (jnp.log(w) + (u - (w - F32(1.0))))


def softplus2(x):
    v = jnp.exp2(jnp.minimum(x, F32(100.0)))
    log = lax.log2(F32(1.0 + 2.0**-23) + v)
    return jnp.maximum(jnp.minimum(log, v * F32(LOG2E)), x)


def sigmoid(x):
    u = jnp.exp(-jnp.abs(x))
    return jnp.where(x >= 0, F32(1.0), u) / (F32(1.0) + u)


def forward_kernel(
    geo_ref, entry_ref, counts_ref, tgt_ref, win_ref, wmid_ref, wout_ref, bhid_ref, bout_ref, freqs_ref,
    send_ref, wb_ref, wob_ref, out_ref, fh_ref, fl_ref, h1h_ref, h1l_ref, h2h_ref, h2l_ref, h3h_ref, h3l_ref, s1_ref, s2_ref, s3_ref,
    wcat, wo, bias, rot, feat, before, color,
    *, delta,
):
    step = pl.program_id(0)

    @pl.when(step == 0)
    def _():
        for i in range(3):
            w = win_ref[0] * F32(LOG2E) if i == 0 else wmid_ref[0, i - 1]
            hi, lo = split(w.T)
            wcat[i, :, 0:256] = hi
            wcat[i, :, 256:512] = hi
            wcat[i, :, 512:768] = lo
            bias[i] = jnp.broadcast_to(bhid_ref[i] * F32(LOG2E), (128, H)).T
        w8 = jnp.concatenate([wout_ref[0] * F32(LN2), jnp.zeros((4, H), F32)], axis=0)
        hi, lo = split(w8)
        wo[...] = jnp.concatenate([hi.astype(F32), lo.astype(F32)], axis=0).astype(BF16)
        for i in range(2):
            hi, lo = split(wmid_ref[0, i])
            wb_ref[i, :, 0:256] = hi
            wb_ref[i, :, 256:512] = hi
            wb_ref[i, :, 512:768] = lo
        w8 = jnp.concatenate([wout_ref[0], jnp.zeros((4, H), F32)], axis=0)
        hi, lo = split(w8)
        hi, lo = hi.astype(F32), lo.astype(F32)
        wob_ref[...] = jnp.concatenate([hi, hi, lo, jnp.zeros((104, H), F32)], axis=0).T[:, 0:32].astype(BF16)
        ft = jnp.concatenate([freqs_ref[0], freqs_ref[1], freqs_ref[2], jnp.zeros((5, FE), F32)], axis=0).T
        geo = geo_ref[:, 0, :]
        a = ft[:, 0:1] * geo[0:1] + ft[:, 1:2] * geo[1:2] + ft[:, 2:3] * geo[2:3]
        d = ft[:, 0:1] * geo[3:4] + ft[:, 1:2] * geo[4:5] + ft[:, 2:3] * geo[5:6]
        t0 = F32(0.25) * (entry_ref[0].astype(F32) + F32(0.5))
        s, c = sincos(a + t0 * d)
        feat[0:FE] = s
        feat[FE:] = c
        s, c = sincos(F32(0.25) * d)
        rot[0:FE] = s
        rot[FE:] = c
        before[...] = jnp.zeros_like(before)
        color[...] = jnp.zeros_like(color)

    n = step * SF

    def slot_input(j):
        s, c = feat[0:FE], feat[FE:]
        fh_ref[n + j, 0:FE], fl_ref[n + j, 0:FE] = split(s)
        fh_ref[n + j, FE:], fl_ref[n + j, FE:] = split(c)
        rs, rc = rot[0:FE], rot[FE:]
        feat[0:FE] = s * rc + c * rs
        feat[FE:] = c * rc - s * rs

    for j in range(SF):
        slot_input(j)
    srcs = [(fh_ref, fl_ref), (h1h_ref, h1l_ref), (h2h_ref, h2l_ref), (h3h_ref, h3l_ref)]
    sigs = [s1_ref, s2_ref, s3_ref]
    parts = [(j, k) for j in range(SF) for k in range(2)]
    for i in range(3):
        b = jnp.concatenate([bias[i], bias[i]], axis=1)
        for j, k in parts:
            lanes = slice(256 * k, 256 * k + 256)
            hi = srcs[i][0][n + j, :, lanes]
            lo = srcs[i][1][n + j, :, lanes]
            x = mm(wcat[i], jnp.concatenate([hi, lo, hi], axis=0)) + b
            h = softplus2(x)
            sigs[i][n + j, :, lanes] = jnp.exp2(x - h)
            srcs[i + 1][0][n + j, :, lanes], srcs[i + 1][1][n + j, :, lanes] = split(h)
    bo = jnp.concatenate([bout_ref[0:1, :], jnp.zeros((1, 124), F32)], axis=1)
    bo = jnp.broadcast_to(bo, (128, 128)).T[0:8, 0:1]
    for j in range(SF):
        d1 = mm(wo[...], h3h_ref[n + j])
        d2 = mm(wo[...], h3l_ref[n + j])
        o = d1[0:8] + d1[8:16] + d2[0:8] + d2[8:16] + bo
        gate = jnp.where(step * SF + j < counts_ref[0], F32(delta), F32(0.0))
        depth = softplus(o[0:1]) * gate
        bef = before[...]
        w = jnp.exp(-bef) * (F32(1.0) - jnp.exp(-depth))
        sg = sigmoid(o)
        color[...] += w * sg
        before[...] = bef + depth
        out_ref[step * SF + j] = jnp.concatenate([sg[0:4], w, jnp.exp(-(bef + depth)), gate, jnp.zeros_like(w)], axis=0)

    @pl.when(step == NF - 1)
    def _():
        t = tgt_ref[:, 0, :]
        t = jnp.concatenate([t[0:1], t[1:2], t[2:3], jnp.zeros((1, 80), F32)], axis=1)
        t = pltpu.roll(jnp.broadcast_to(t, (8, 128)), lax.rem(lax.axis_index("slab"), 8) * OWN, 1)[0:1]
        rows = []
        for c in range(4):
            v = color[c + 1 : c + 2] if c < 3 else -before[...]
            rows += [v[:, 128 * q : 128 * q + 128] for q in range(4)]
        rows.append(t)
        value = jnp.concatenate(rows, axis=0)
        for s in range(32):
            send_ref[s * ROWS : (s + 1) * ROWS] = value


def where():
    ray = lax.axis_index("rays")
    return lax.rem(ray, 2), lax.div(ray, 2)


def keep(x):
    return pltpu.with_memory_space_constraint(x, pltpu.VMEM)


def vmem():
    return pl.BlockSpec(memory_space=pltpu.VMEM)


def full(shape):
    return pl.BlockSpec(shape, lambda i, n=len(shape): (0,) * n)


def forward(geo, entry, counts, tgt, w_in, w_mid, w_out, b_hid, b_out, freqs, delta):
    res = [jax.ShapeDtypeStruct((32 * ROWS, 128), F32), pltpu.VMEM((2, H, 3 * H), BF16), pltpu.VMEM((H, 32), BF16), pltpu.VMEM((SAMP, 8, RAYS), F32)]
    res += [pltpu.VMEM((SAMP, H, RAYS), BF16)] * 8 + [pltpu.VMEM((SAMP, H, RAYS), F32)] * 3
    return pl.pallas_call(
        lambda *refs: forward_kernel(*refs, delta=delta),
        grid=(NF,),
        in_specs=[full(x.shape) for x in (geo, entry, counts, tgt, w_in, w_mid, w_out, b_hid, b_out, freqs)],
        out_specs=[full((32 * ROWS, 128))] + [vmem()] * 14,
        out_shape=res,
        scratch_shapes=[
            pltpu.VMEM((3, H, 3 * H), BF16), pltpu.VMEM((16, H), BF16),
            pltpu.VMEM((3, H, 128), F32), pltpu.VMEM((H, RAYS), F32), pltpu.VMEM((H, RAYS), F32),
            pltpu.VMEM((1, RAYS), F32), pltpu.VMEM((8, RAYS), F32),
        ],
        compiler_params=pltpu.CompilerParams(vmem_limit_bytes=28 * 1024 * 1024),
        name="fwd",
    )(geo, entry, counts, tgt, w_in, w_mid, w_out, b_hid, b_out, freqs)


def backward_kernel(
    recv_ref, wcat, wo, out_ref,
    fh_ref, fl_ref, h1h_ref, h1l_ref, h2h_ref, h2l_ref, h3h_ref, h3l_ref, s1_ref, s2_ref, s3_ref,
    pix_ref, mine_ref, other_ref,
    g_all, adj, pixs, acc, bacc, gacc, goacc, dh_buf,
    *, factor,
):
    step = pl.program_id(0)

    @pl.when(step == 0)
    def _():
        me = lax.axis_index("slab")
        acc[...] = jnp.zeros_like(acc)
        bacc[...] = jnp.zeros_like(bacc)
        gacc[...] = jnp.zeros_like(gacc)
        goacc[...] = jnp.zeros_like(goacc)
        zero = jnp.zeros((4, 128), F32)
        depth, own, pix, after = zero, zero, [zero] * 3, [zero] * 3
        for s in range(32):
            shade = jnp.exp(depth)
            own = jnp.where(me == s, shade, own)
            late = jnp.where(s > me, F32(1.0), F32(0.0))
            for c in range(3):
                part = shade * recv_ref[s * ROWS + 4 * c : s * ROWS + 4 * c + 4]
                pix[c] = pix[c] + part
                after[c] = after[c] + late * part
            depth = depth + recv_ref[s * ROWS + 12 : s * ROWS + 16]
        through = jnp.exp(depth)
        lane = lax.broadcasted_iota(jnp.int32, (8, 128), 1)
        sub = lax.broadcasted_iota(jnp.int32, (8, 128), 0)
        adj[...] = jnp.zeros_like(adj)
        log_adj = zero
        for c in range(3):
            rows = []
            for q in range(4):
                t = jnp.concatenate(
                    [recv_ref[(8 * q + s) * ROWS + 16 : (8 * q + s) * ROWS + 17] for s in range(8)], axis=0
                )
                if c:
                    t = pltpu.roll(t, 128 - OWN * c, 1)
                t = jnp.where(lax.div(lane, OWN) == sub, t, F32(0.0))
                rows.append(jnp.sum(t, axis=0, keepdims=True))
            target = jnp.concatenate(rows, axis=0)
            pixel = pix[c] + through
            pixs[4 * c : 4 * c + 4] = pixel
            dpix = F32(2.0 * factor) * (pixel - target)
            log_adj = log_adj + dpix * (after[c] + through)
            a = own * dpix
            for q in range(4):
                adj[c + 1 : c + 2, 128 * q : 128 * q + 128] = a[q : q + 1]
        for c in range(3):
            row = pixs[pl.ds(4 * c + lax.div(me, 8), 1), :]
            row = pltpu.roll(jnp.broadcast_to(row, (8, 128)), lax.rem(128 - lax.rem(me, 8) * OWN, 128), 1)
            pix_ref[c] = row[0:1, 0:OWN]
        log_adj = jnp.concatenate([log_adj[q : q + 1] for q in range(4)], axis=1)
        a8 = adj[...]
        later = jnp.zeros((8, RAYS), F32)
        first = lax.broadcasted_iota(jnp.int32, (8, RAYS), 0) == 0
        for j in reversed(range(SAMP)):
            sg = out_ref[j]
            w, end, gate = sg[4:5], sg[5:6], sg[6:7]
            ddep = gate * (jnp.sum(a8 * (end * sg - later), axis=0, keepdims=True) - log_adj)
            g = jnp.where(first, ddep * sg, a8 * w * (sg * (F32(1.0) - sg)))
            later = later + w * sg
            g_all[j] = g

    n = step * SB
    gout = []
    for j in range(SB):
        g = g_all[step * SB + j]
        gacc[...] += g[:, 0:128] + g[:, 128:256] + g[:, 256:384] + g[:, 384:512]
        gh, gl = split(g)
        gh, gl = gh.astype(F32), gl.astype(F32)
        gk = jnp.concatenate([gh, gl, gh, jnp.zeros((8, RAYS), F32)], axis=0).astype(BF16)
        g16 = jnp.concatenate([gh, gl], axis=0).astype(BF16)
        d = mm_nt(jnp.concatenate([g16, g16], axis=1), jnp.concatenate([h3h_ref[n + j], h3l_ref[n + j]], axis=1))
        gout.append(d[0:8] + d[8:16])
        dh_buf[j] = mm(wo[...], gk)
    goacc[...] += sum(gout[1:], gout[0])
    sigs = (s3_ref, s2_ref, s1_ref)
    hs = ((h2h_ref, h2l_ref), (h1h_ref, h1l_ref), (fh_ref, fl_ref))
    for i in range(3):
        lhs, rhs = [], []
        for j in range(SB):
            dx = dh_buf[j] * sigs[i][n + j]
            bacc[2 - i] += dx[:, 0:128] + dx[:, 128:256] + dx[:, 256:384] + dx[:, 384:512]
            xh, xl = split(dx)
            lhs += [hs[i][0][n + j], hs[i][0][n + j], hs[i][1][n + j]]
            rhs += [xh, xl, xh]
            if i < 2:
                dh_buf[j] = mm(wcat[1 - i], jnp.concatenate([xh, xl, xh], axis=0))
        acc[2 - i] += mm_nt(jnp.concatenate(lhs, axis=1), jnp.concatenate(rhs, axis=1))

    @pl.when(step == NB - 1)
    def _():
        core, chip = where()
        for k in range(4):
            q = lax.rem(chip + k, 4)
            for i in range(3):
                rows = pl.ds(96 * k + 32 * i, 32)
                unit = F32(LN2 if i else 1.0)
                mine_ref[rows] = acc[i, pl.ds((core * 4 + q) * 32, 32), :] * unit
                other_ref[rows] = acc[i, pl.ds(((1 - core) * 4 + q) * 32, 32), :] * unit
        lane = lax.broadcasted_iota(jnp.int32, (8, 128), 1)
        sub = lax.broadcasted_iota(jnp.int32, (8, 128), 0)
        hid = [jnp.sum(bacc[i].T, axis=0, keepdims=True) for i in range(3)]
        gb = jnp.broadcast_to(jnp.sum(gacc[...], axis=1, keepdims=True), (8, 128))
        gb = jnp.sum(jnp.where(lane == sub, gb, F32(0.0)), axis=0, keepdims=True)
        gb = jnp.concatenate([gb, jnp.zeros((1, 128), F32)], axis=1)
        small = jnp.concatenate([goacc[0:4] * F32(LN2)] + hid + [gb], axis=0)
        mine_ref[384:392] = small
        other_ref[384:392] = small


def backward(recv, wb, wo, out, residuals, factor):
    args = [keep(x) for x in (recv, wb, wo, out, *residuals)]
    return pl.pallas_call(
        lambda *refs: backward_kernel(*refs, factor=factor),
        grid=(NB,),
        in_specs=[vmem()] * len(args),
        out_specs=[vmem()] * 3,
        out_shape=[pltpu.VMEM((3, 1, OWN), F32), pltpu.VMEM((392, H), F32), pltpu.VMEM((392, H), F32)],
        scratch_shapes=[
            pltpu.VMEM((SAMP, 8, RAYS), F32), pltpu.VMEM((8, RAYS), F32), pltpu.VMEM((16, 128), F32),
            pltpu.VMEM((3, H, H), F32), pltpu.VMEM((3, H, 128), F32), pltpu.VMEM((8, 128), F32), pltpu.VMEM((8, H), F32),
            pltpu.VMEM((SB, H, RAYS), F32),
        ],
        compiler_params=pltpu.CompilerParams(vmem_limit_bytes=24 * 1024 * 1024),
        name="bwd",
    )(*args)


def copies(side, sources, gin, gmid, sem):
    core, chip = where()
    started = []
    for n, k in enumerate(ORDER):
        q = lax.rem(chip + 4 - k, 4)
        rows = pl.ds(((core if side == 0 else 1 - core) * 4 + q) * 32, 32)
        src, base = sources(n)
        for i, dst in enumerate((gin.at[0, rows], gmid.at[0, 0, rows], gmid.at[0, 1, rows])):
            copy = pltpu.make_async_copy(src.at[pl.ds(base + 32 * i, 32)], dst, sem.at[3 * n + i])
            copy.start()
            started.append(copy)
    return started


def place_own_kernel(done, own_a, own_b, own_c, gin, gmid, gout, ghid, gbout, sem):
    own = (done, own_a, own_b, own_c)
    started = copies(0, lambda k: (own[k], 0), gin, gmid, sem)
    gout[0] = done[96:100]
    for i in range(3):
        ghid[i] = done[100 + i : 101 + i]
    gbout[...] = done[103:104, 0:4]
    for copy in started:
        copy.wait()


def place_other_kernel(sib, gin_in, gmid_in, gin, gmid, sem):
    for copy in copies(1, lambda k: (sib, 96 * k), gin, gmid, sem):
        copy.wait()


def hbm():
    return pl.BlockSpec(memory_space=pl.ANY)


def place_own(done, own):
    shapes = [(1, H, H), (1, 2, H, H), (1, 4, H), (3, 1, H), (1, 4)]
    return pl.pallas_call(
        place_own_kernel,
        in_specs=[vmem()] * 4,
        out_specs=[hbm()] * 2 + [vmem()] * 3,
        out_shape=[jax.ShapeDtypeStruct(x, F32) for x in shapes],
        scratch_shapes=[pltpu.SemaphoreType.DMA((12,))],
        compiler_params=pltpu.CompilerParams(vmem_limit_bytes=16 * 1024 * 1024),
        name="place_own",
    )(*[keep(x) for x in (done, *own)])


def place_other(sib, gin, gmid):
    return pl.pallas_call(
        place_other_kernel,
        in_specs=[vmem()] + [hbm()] * 2,
        out_specs=[hbm()] * 2,
        out_shape=[jax.ShapeDtypeStruct(x.shape, F32) for x in (gin, gmid)],
        scratch_shapes=[pltpu.SemaphoreType.DMA((12,))],
        input_output_aliases={1: 0, 2: 1},
        compiler_params=pltpu.CompilerParams(vmem_limit_bytes=16 * 1024 * 1024),
        name="place_other",
    )(keep(sib), gin, gmid)


def shards(geometry, entry, counts, targets, w_in, w_mid, w_out, b_hid, b_out, freqs):
    slabs = lax.axis_size("slab")
    delta = 3.0 / (SAMP * slabs)
    factor = 1.0 / math.sqrt(3.0 * lax.axis_size("rays") * slabs * OWN)
    send, wb, wo, out, *residuals = forward(
        geometry, entry, counts, targets, w_in, w_mid, w_out,
        b_hid.transpose(1, 0, 2), b_out, freqs.transpose(1, 0, 2), delta
    )
    recv = lax.all_to_all(send.reshape(32, 1, ROWS * 128), "slab", 0, 0, tiled=True).reshape(32 * ROWS, 128)
    pixels, mine, other = backward(recv, wb, wo, out, residuals, factor)
    swap = [(i, i ^ 1) for i in range(8)]
    along = [[(i, (i + 2 * k) % 8) for i in range(8)] for k in range(4)]
    total = mine + lax.ppermute(other, "rays", swap)
    small = total[384:392]
    parts = [jnp.concatenate([total[96 * k : 96 * k + 96], small], axis=0) for k in range(4)]
    got = [lax.ppermute(parts[k], "rays", along[k]) for k in range(1, 4)]
    done = parts[0] + got[0] + got[1] + got[2]
    chunk = done[0:96]
    own = [lax.ppermute(chunk, "rays", along[k]) for k in ORDER[1:]]
    sib = lax.ppermute(jnp.concatenate([chunk] + own, axis=0), "rays", swap)
    grad_in, grad_mid, grad_out, grad_hid, grad_bout = place_own(done, own)
    grad_in, grad_mid = place_other(sib, grad_in, grad_mid)
    return pixels, grad_in, grad_mid, grad_out, grad_hid.transpose(1, 0, 2), grad_bout


def solution(mesh):
    in_specs = (
        P(None, "rays", None),
        P("slab", "rays", None),
        P("slab", "rays", None),
        P(None, "rays", "slab"),
        P("slab", None, None),
        P("slab", None, None, None),
        P("slab", None, None),
        P("slab", None, None),
        P("slab", None),
        P("slab", None, None),
    )
    out_specs = (
        P(None, "rays", "slab"),
        P("slab", None, None),
        P("slab", None, None, None),
        P("slab", None, None),
        P("slab", None, None),
        P("slab", None),
    )
    return jax.shard_map(shards, mesh=mesh, in_specs=in_specs, out_specs=out_specs, check_vma=False)
```
